256 devices in a mesh: groups: 2 (over y), ep: 16 (over z), tp: 4 (over x), dp: 2 (over core).
Axes of the slice: x: 4, y: 2, z: 16, core: 2. Of those that a mesh axis runs over, the one named last changes fastest.
The devices are a block of a 4x16x16 slice.
Arguments:
- hidden: bfloat16 [2048, 7168], P(('groups', 'ep', 'tp', 'dp')), parts along dimension 0, may hold values from -6 to 6
- norm_gain: bfloat16 [7168], replicated, may hold values from 0.099609375 to 1.8984375
- router: bfloat16 [7168, 32], replicated, may hold values from -0.0625 to 0.0625
- expert_ids: int32 [2048, 8], P(('groups', 'ep', 'tp', 'dp')), parts along dimension 0, may hold values from 0 to 31, all different within a row; in each aligned block of 4 rows (0 to 3, 4 to 7, ...) at most 2 rows name the same one
- gate_proj: bfloat16 [32, 7168, 1024], P(('ep', 'dp'), None, 'tp'), may hold values from -0.0625 to 0.0625
- up_proj: bfloat16 [32, 7168, 1024], P(('ep', 'dp'), None, 'tp'), may hold values from -0.0625 to 0.0625
- down_proj: bfloat16 [32, 1024, 7168], P(('ep', 'dp'), 'tp'), may hold values from -0.1875 to 0.1875
Outputs:
- mixed: bfloat16 [2048, 7168], P(('groups', 'ep', 'tp', 'dp')), parts along dimension 0
The draws below stay inside these ranges and needn't reach their ends.
There are 2 independent parts, one for each index of `groups`. The reference program is written for one: setup_inputs(seed, part) draws one part's arguments, and reference() takes and returns one part's arrays. A program takes and returns all parts, laid end to end along the dimension named above; an argument that names none is the same for every part. Nothing has to cross between parts.
Inputs may be any that keep to these rules, and one draw needn't show every extreme that they name: `expert_ids`: each row names 8 different experts. In each aligned block of 4 rows (one micro-batch of one device) no expert is named by more than 2 rows, a bound that some block reaches.
All inputs are finite; a program needn't handle non-finite values.
Results may differ from the reference program's by a relative error of at most 0.008.
Values may be sent and summed in bfloat16 or wider, within the bound.
No kernel may reach another device: no remote copies, remote signals or barrier semaphores. Data moves between devices by JAX's collectives and lax.ppermute only.
A program may use at most 128 MiB of HBM per device.

```python
import math
import jax
import jax.numpy as jnp
import numpy as np
from jax import lax

D = 7168
FF_EXPERT = 1024
TOP = 8
MB_ROWS = 4
EXPERTS = 32
CAP = 2
TOKENS = 1024
N_TP = 4


def block_levels(stream_key, extent, shards, low, high):
    factor_of = 1.0
    for position, blocks in shards:
        heights = jax.random.uniform(jax.random.fold_in(jax.random.fold_in(stream_key, 6), position), (blocks,), jnp.float32, low / len(shards), high / len(shards))
        factor_of = factor_of * jnp.repeat(jnp.exp(heights), extent[position] // blocks).reshape((-1,) + (1,) * (len(extent) - 1 - position))
    return factor_of


def routed_block(stream_key, own, number, rows, count, top, most, slope):
    ranking = jax.random.permutation(stream_key, count)
    heavy_load, usual = shares(count, rows * top, most, slope, True), shares(count, rows * top, most, slope, False)
    places = jnp.arange(count)

    def named(sizes, offset_by):
        used = int((sizes > 0).sum())
        fixed = max(1, used // 4)
        passed = fixed + (places - fixed + offset_by * (used - fixed)) % max(1, count - fixed)
        return jnp.zeros((count,), jnp.int32).at[ranking[jnp.where(places < fixed, places, passed)]].set(jnp.asarray(sizes, jnp.int32))

    sizes = jnp.where(number % 4 == 0, named(heavy_load, number // 4), named(usual, number - number // 4 - 1))
    mixed = jax.random.permutation(jax.random.fold_in(own, 3), count)
    giver, receiver = mixed[0:count // 2 * 2:2], mixed[1:count // 2 * 2:2]
    slack = jnp.minimum(sizes[giver] - 1, most - sizes[receiver]) // 2
    slack = jnp.where((giver == ranking[0]) | (receiver == ranking[0]) | (sizes[receiver] == 0), 0, jnp.maximum(slack, 0))
    passed = jax.random.randint(jax.random.fold_in(own, 4), (count // 2,), 0, 1 << 20) % (slack + 1)
    sizes = sizes.at[giver].add(-passed).at[receiver].add(passed)
    members = jnp.searchsorted(jnp.cumsum(sizes), jnp.arange(rows * top), side="right").astype(jnp.int32)
    listing = members.reshape(top, rows).T
    listing = listing[jax.random.permutation(jax.random.fold_in(own, 1), rows)]
    offset_by = jax.random.randint(jax.random.fold_in(own, 2), (rows, 1), 0, top)
    return jnp.take_along_axis(listing, (jnp.arange(top)[None, :] + offset_by) % top, axis=1)


def shares(amount, total, limit, lean, full):
    weights = [(1 << 20) // math.isqrt(grade ** lean) + 1 for grade in range(1, amount + 1)]
    largest = limit if full else min(limit, max(-(-total // amount), total * weights[0] // sum(weights)))
    least = 1 if total - largest >= amount - 1 else 0
    given, surplus = [largest] + [least] * (amount - 1), total - largest - least * (amount - 1)
    while surplus > 0:
        free = [i for i in range(1, amount) if given[i] < largest] or [i for i in range(1, amount) if given[i] < limit]
        pool, remaining = sum([weights[i] for i in free]), surplus
        for i in free:
            extra = min(limit - given[i], max(1, remaining * weights[i] // pool), surplus)
            given[i] = given[i] + extra
            surplus = surplus - extra
    return np.array(given)


def noise(key, extent, scale, bound, split=(), kind=jnp.bfloat16):
    entries = jax.random.normal(key, extent, jnp.float32) * scale
    if len(split) > 0:
        entries = block_levels(key, extent, split, -0.22, 0.18) * entries
    return jnp.clip(entries, min=-bound, max=bound).astype(kind)


def setup_inputs(seed: int = 0, part: int = 0) -> dict:
    seeds = jax.random.split(jax.random.key(seed), 8)
    part_keys = jax.random.split(jax.random.fold_in(seeds[7], part), 8)
    hidden = noise(part_keys[0], (TOKENS, D), 1.0, 6.0, ((0, 128),))
    norm_gain = jnp.clip(1.0 + 0.18 * jax.random.normal(seeds[1], (D,), jnp.float32), 0.099609375, 1.8984375).astype(jnp.bfloat16)
    router = noise(seeds[2], (D, EXPERTS), D ** -0.5, 0.0625)
    expert_ids_keys = jax.random.split(jax.random.fold_in(part_keys[3], 1), TOKENS // MB_ROWS)
    expert_ids_turns = jax.random.permutation(jax.random.fold_in(part_keys[3], 3), TOKENS // MB_ROWS)
    expert_ids = jax.vmap(lambda own, number: routed_block(jax.random.fold_in(part_keys[3], 2), own, number, MB_ROWS, EXPERTS, TOP, CAP, 2))(expert_ids_keys, expert_ids_turns).reshape((TOKENS, TOP))
    gate_proj = noise(seeds[4], (EXPERTS, D, FF_EXPERT), D ** -0.5, 0.0625, ((0, 32), (2, 4)))
    up_proj = noise(seeds[5], (EXPERTS, D, FF_EXPERT), D ** -0.5, 0.0625, ((0, 32), (2, 4)))
    down_proj = noise(seeds[6], (EXPERTS, FF_EXPERT, D), FF_EXPERT ** -0.5, 0.1875, ((0, 32), (1, 4)))
    return {"hidden": hidden, "norm_gain": norm_gain, "router": router, "expert_ids": expert_ids, "gate_proj": gate_proj, "up_proj": up_proj, "down_proj": down_proj}


route_scale = 2.827
norm_eps = 1e-06

def normalize(hidden, norm_gain):
    values = hidden.astype(jnp.float32)
    spread = lax.optimization_barrier(jnp.mean(values * values, axis=-1, keepdims=True))
    return (values * lax.rsqrt(spread + norm_eps) * norm_gain.astype(jnp.float32)).astype(jnp.bfloat16)

def reference(hidden, norm_gain, router, expert_ids, gate_proj, up_proj, down_proj):
    normed = normalize(hidden, norm_gain)
    logits = jnp.dot(normed, router, preferred_element_type=jnp.float32)
    scores = jax.nn.sigmoid(logits)
    chosen = jnp.take_along_axis(scores, expert_ids, axis=1)
    weights = route_scale * chosen / lax.optimization_barrier(jnp.sum(chosen, axis=1, keepdims=True))
    block_count = TOKENS // MB_ROWS
    block_ids = expert_ids.reshape(block_count, MB_ROWS * TOP)
    onehot = (block_ids[:, :, None] == jnp.arange(EXPERTS, dtype=jnp.int32)[None, None, :]).astype(jnp.int32)
    earlier = jnp.cumsum(onehot, axis=1) - onehot
    slot_rank = lax.optimization_barrier(jnp.sum(earlier * onehot, axis=2)).astype(jnp.int32)
    token_index = (jnp.arange(block_count, dtype=jnp.int32)[:, None] * MB_ROWS + jnp.arange(MB_ROWS * TOP, dtype=jnp.int32)[None, :] // TOP).astype(jnp.int32)
    column = (jnp.arange(block_count, dtype=jnp.int32)[:, None] * CAP + slot_rank).astype(jnp.int32)
    table = jnp.full((EXPERTS, block_count * CAP), TOKENS, dtype=jnp.int32)
    table = table.at[block_ids, column].set(token_index)
    padded = jnp.concatenate([normed, jnp.zeros((1, D), normed.dtype)], axis=0)

    def one_expert(operands):
        rows_index, gate_w, up_w, down_w = operands
        row_block = padded[rows_index].astype(jnp.float32)
        gate_sum = jnp.dot(row_block, gate_w.astype(jnp.float32), precision=lax.Precision.HIGHEST)
        up_sum = jnp.dot(row_block, up_w.astype(jnp.float32), precision=lax.Precision.HIGHEST)
        active = (jax.nn.silu(gate_sum) * up_sum).astype(jnp.bfloat16)
        split_active = active.reshape(-1, N_TP, FF_EXPERT // N_TP).astype(jnp.float32)
        split_down = down_w.reshape(N_TP, FF_EXPERT // N_TP, D).astype(jnp.float32)
        quarters = jnp.einsum('rqf,qfd->qrd', split_active, split_down, precision=lax.Precision.HIGHEST)
        rounded = lax.optimization_barrier(quarters.astype(jnp.bfloat16))
        return lax.optimization_barrier(jnp.sum(rounded.astype(jnp.float32), axis=0)).astype(jnp.bfloat16)
    expert_out = lax.map(one_expert, (table, gate_proj, up_proj, down_proj))
    pick_column = column.reshape(TOKENS, TOP)
    picked = expert_out[expert_ids, pick_column]
    expert_sum = lax.optimization_barrier(jnp.sum(weights[:, :, None] * picked.astype(jnp.float32), axis=1))
    return (hidden.astype(jnp.float32) + expert_sum).astype(jnp.bfloat16)
```

```python
import jax
import jax.numpy as jnp
from jax import lax
from jax.sharding import PartitionSpec as P

GROUP = ("ep", "tp", "dp")
LANES = 128

route_scale = 2.827
norm_eps = 1e-06


def normalize(hidden, norm_gain):
    values = hidden.astype(jnp.float32)
    spread = jnp.mean(values * values, axis=-1, keepdims=True)
    return (values * lax.rsqrt(spread + norm_eps) * norm_gain.astype(jnp.float32)).astype(
        jnp.bfloat16
    )


def dense_weights(normed, router, expert_ids):
    logits = jnp.dot(normed, router, preferred_element_type=jnp.float32)
    scores = jax.nn.sigmoid(logits)
    expert_range = jnp.arange(router.shape[1], dtype=jnp.int32)
    chosen = jnp.any(expert_ids[:, :, None] == expert_range[None, None, :], axis=1)
    chosen_scores = jnp.where(chosen, scores, 0.0)
    return route_scale * chosen_scores / jnp.sum(chosen_scores, axis=-1, keepdims=True)


def weight_columns(weights):
    high = lax.reduce_precision(weights, exponent_bits=8, mantissa_bits=7)
    low = weights - high
    columns = jnp.concatenate([high, low], axis=1).astype(jnp.bfloat16)
    return jnp.pad(columns, ((0, 0), (0, LANES - columns.shape[1])))


def body(hidden, norm_gain, router, expert_ids, gate_proj, up_proj, down_proj):
    features = hidden.shape[1]
    experts = router.shape[1]
    normed = normalize(hidden, norm_gain)
    weights = dense_weights(normed, router, expert_ids)
    outgoing = jnp.concatenate([normed, weight_columns(weights)], axis=1)
    everyone = lax.all_gather(outgoing, GROUP, axis=0, tiled=True)
    rows = everyone[:, :features]
    own = lax.axis_index("ep") * lax.axis_size("dp") + lax.axis_index("dp")
    lane = jnp.arange(LANES, dtype=jnp.int32)
    own_lanes = (lane == own) | (lane == own + experts)
    columns = everyone[:, features:].astype(jnp.float32)
    weight = jnp.sum(jnp.where(own_lanes, columns, 0.0), axis=1, keepdims=True)
    gate_sum = jnp.dot(rows, gate_proj[0], preferred_element_type=jnp.float32)
    up_sum = jnp.dot(rows, up_proj[0], preferred_element_type=jnp.float32)
    active = (weight * (jax.nn.silu(gate_sum) * up_sum)).astype(jnp.bfloat16)
    partial_rows = jnp.dot(active, down_proj[0], preferred_element_type=jnp.float32)
    expert_sum = lax.psum_scatter(
        partial_rows.astype(jnp.bfloat16), GROUP, scatter_dimension=0, tiled=True
    )
    return (hidden.astype(jnp.float32) + expert_sum.astype(jnp.float32)).astype(jnp.bfloat16)


def solution(mesh):
    return jax.shard_map(
        body,
        mesh=mesh,
        in_specs=(
            P(("groups", "ep", "tp", "dp"), None),
            P(),
            P(),
            P(("groups", "ep", "tp", "dp"), None),
            P(("ep", "dp"), None, "tp"),
            P(("ep", "dp"), None, "tp"),
            P(("ep", "dp"), "tp", None),
        ),
        out_specs=P(("groups", "ep", "tp", "dp"), None),
        check_vma=False,
    )
```

```python
import jax
import jax.numpy as jnp
from jax import lax
from jax.sharding import PartitionSpec as P


MB_ROWS = 4
CAP = 2
LANES = 128
REACHES = (3, 6, 8)
PIECES = len(REACHES)

route_scale = 2.827
norm_eps = 1e-06


def normalize(hidden, norm_gain):
    values = hidden.astype(jnp.float32)
    spread = jnp.mean(values * values, axis=-1, keepdims=True)
    return (values * lax.rsqrt(spread + norm_eps) * norm_gain.astype(jnp.float32)).astype(
        jnp.bfloat16
    )


def dense_weights(normed, router, expert_ids):
    logits = jnp.dot(normed, router, preferred_element_type=jnp.float32)
    scores = jax.nn.sigmoid(logits)
    expert_range = jnp.arange(router.shape[1], dtype=jnp.int32)
    chosen = jnp.any(expert_ids[:, :, None] == expert_range[None, None, :], axis=1)
    chosen_scores = jnp.where(chosen, scores, 0.0)
    weights = route_scale * chosen_scores / jnp.sum(chosen_scores, axis=-1, keepdims=True)
    return chosen.astype(jnp.float32), weights


def tag_columns(chosen, weights):
    high = lax.reduce_precision(weights, exponent_bits=8, mantissa_bits=7)
    columns = jnp.concatenate([chosen, high, weights - high], axis=1)
    width = columns.shape[1]
    return jnp.pad(columns, ((0, 0), (0, -width % LANES))).astype(jnp.bfloat16)


def shift(value, axis, step):
    size = lax.axis_size(axis)
    return lax.ppermute(value, axis, [(i, (i + step) % size) for i in range(size)])


def add(*terms):
    return sum(term.astype(jnp.float32) for term in terms).astype(jnp.bfloat16)


def slot_maps(tags, own, experts, first_block, blocks):
    rows = tags.shape[0]
    lane = jnp.arange(tags.shape[1], dtype=jnp.int32)
    values = tags.astype(jnp.float32)
    chosen = jnp.sum(jnp.where(lane == own, values, 0.0), axis=1)
    weighing = (lane == own + experts) | (lane == own + 2 * experts)
    weight = jnp.sum(jnp.where(weighing, values, 0.0), axis=1)
    row = jnp.arange(rows, dtype=jnp.int32)
    earlier = (row[:, None] // MB_ROWS == row[None, :] // MB_ROWS) & (row[None, :] < row[:, None])
    rank = jnp.sum(jnp.where(earlier, chosen[None, :], 0.0), axis=1)
    slot = jnp.arange(blocks * CAP, dtype=jnp.int32)
    same_block = slot[:, None] // CAP == first_block + row[None, :] // MB_ROWS
    same_rank = (slot % CAP).astype(jnp.float32)[:, None] == rank[None, :]
    hits = same_block & same_rank & (chosen[None, :] > 0.5)
    return hits.astype(jnp.bfloat16), weight[:, None]


def matmul(left, right):
    return jnp.dot(left, right, preferred_element_type=jnp.float32)


def expert(rows, gate_proj, up_proj, down_proj):
    gate_sum = matmul(rows, gate_proj)
    up_sum = matmul(rows, up_proj)
    active = (jax.nn.silu(gate_sum) * up_sum).astype(jnp.bfloat16)
    active = lax.optimization_barrier(active)
    return matmul(active, down_proj).astype(jnp.bfloat16)


def body(hidden, norm_gain, router, expert_ids, gate_proj, up_proj, down_proj):
    tokens, features = hidden.shape
    experts = router.shape[1]
    ring = lax.axis_size("ep")
    reach = ring // 2
    own = lax.axis_index("ep") * lax.axis_size("dp") + lax.axis_index("dp")
    normed = normalize(hidden, norm_gain)
    tagged = jnp.concatenate(
        [normed, tag_columns(*dense_weights(normed, router, expert_ids))], axis=1
    )

    sources = [[(0, 0)] if piece == 0 else [] for piece in range(PIECES)]
    blocks = {(0, 0): tagged}
    lower = upper = tagged
    for distance in range(1, reach + 1):
        piece = next(p for p in range(PIECES) if distance <= REACHES[p])
        lower = shift(lower, "ep", 1)
        blocks[distance, 0] = lower
        sources[piece].append((distance, 0))
        if distance < ring - distance:
            upper = shift(upper, "ep", -1)
            blocks[distance, 1] = upper
            sources[piece].append((distance, 1))

    half = features // 2
    gathered = []
    for piece in range(PIECES):
        mine = jnp.concatenate([blocks[source] for source in sources[piece]], axis=0)
        other = shift(mine, "dp", 1)
        count = mine.shape[0] // MB_ROWS
        maps = [
            slot_maps(part[:, features:], own, experts, index * count, 2 * count)
            for index, part in enumerate((mine, other))
        ]
        slots = sum(
            matmul(hits, part[:, :features]) for (hits, _), part in zip(maps, (mine, other))
        ).astype(jnp.bfloat16)
        from_left = shift(slots, "tp", 1)
        from_right = shift(slots, "tp", -1)
        far_head = shift(from_left[:, :half], "tp", 1)
        far_tail = shift(from_right[:, half:], "tp", -1)
        far = jnp.concatenate([far_head, far_tail], axis=1)
        gathered.append((maps, (slots, from_left, from_right, far)))

    sums = {}
    for piece in reversed(range(PIECES)):
        maps, parts = gathered[piece]
        rows = jnp.concatenate(parts, axis=0)
        result = expert(rows, gate_proj[0], up_proj[0], down_proj[0])
        own_part, left_part, right_part, far_part = jnp.split(result, 4, axis=0)
        head = shift(far_part[:, :half], "tp", -1)
        tail = shift(far_part[:, half:], "tp", 1)
        left_out = jnp.concatenate([add(left_part[:, :half], head), left_part[:, half:]], axis=1)
        right_out = jnp.concatenate([right_part[:, :half], add(right_part[:, half:], tail)], axis=1)
        from_right = shift(left_out, "tp", -1)
        from_left = shift(right_out, "tp", 1)
        total = add(own_part, from_right, from_left)
        mine, other = [
            weight
            * lax.dot_general(
                hits, total, (((0,), (0,)), ((), ())), preferred_element_type=jnp.float32
            )
            for hits, weight in maps
        ]
        spread = mine + shift(other.astype(jnp.bfloat16), "dp", 1)
        for index, source in enumerate(sources[piece]):
            sums[source] = spread[index * tokens : (index + 1) * tokens]

    lower = upper = None
    for distance in range(reach, 0, -1):
        terms = [sums[distance, 0]]
        if (distance, 1) in sums:
            terms.append(sums[distance, 1])
        if lower is not None:
            terms[0] = terms[0] + lower
        if upper is not None:
            terms[1] = terms[1] + upper
        terms = lax.optimization_barrier([term.astype(jnp.bfloat16) for term in terms])
        lower = shift(terms[0], "ep", -1)
        if len(terms) > 1:
            upper = shift(terms[1], "ep", 1)
    expert_sum = sums[0, 0] + lower + upper
    return (hidden.astype(jnp.float32) + expert_sum).astype(jnp.bfloat16)


def solution(mesh):
    return jax.shard_map(
        body,
        mesh=mesh,
        in_specs=(
            P(("groups", "ep", "tp", "dp"), None),
            P(),
            P(),
            P(("groups", "ep", "tp", "dp"), None),
            P(("ep", "dp"), None, "tp"),
            P(("ep", "dp"), None, "tp"),
            P(("ep", "dp"), "tp", None),
        ),
        out_specs=P(("groups", "ep", "tp", "dp"), None),
        check_vma=False,
    )
```

```python
import jax
import jax.numpy as jnp
from jax import lax
from jax.sharding import PartitionSpec as P


MB_ROWS = 4
CAP = 2
LANES = 128
REACHES = (3, 5, 8)
PIECES = len(REACHES)

route_scale = 2.827
norm_eps = 1e-06


def normalize(hidden, norm_gain):
    values = hidden.astype(jnp.float32)
    spread = jnp.mean(values * values, axis=-1, keepdims=True)
    return (values * lax.rsqrt(spread + norm_eps) * norm_gain.astype(jnp.float32)).astype(
        jnp.bfloat16
    )


def dense_weights(normed, router, expert_ids):
    logits = jnp.dot(normed, router, preferred_element_type=jnp.float32)
    scores = jax.nn.sigmoid(logits)
    expert_range = jnp.arange(router.shape[1], dtype=jnp.int32)
    chosen = jnp.any(expert_ids[:, :, None] == expert_range[None, None, :], axis=1)
    chosen_scores = jnp.where(chosen, scores, 0.0)
    weights = route_scale * chosen_scores / jnp.sum(chosen_scores, axis=-1, keepdims=True)
    return chosen.astype(jnp.float32), weights


def tag_columns(chosen, weights):
    high = lax.reduce_precision(weights, exponent_bits=8, mantissa_bits=7)
    columns = jnp.concatenate([chosen, high, weights - high], axis=1)
    width = columns.shape[1]
    return jnp.pad(columns, ((0, 0), (0, -width % LANES))).astype(jnp.bfloat16)


def shift(value, axis, step):
    size = lax.axis_size(axis)
    return lax.ppermute(value, axis, [(i, (i + step) % size) for i in range(size)])


def add(*terms):
    return sum(term.astype(jnp.float32) for term in terms).astype(jnp.bfloat16)


def slot_maps(tags, own, experts, first_block, blocks):
    rows = tags.shape[0]
    lane = jnp.arange(tags.shape[1], dtype=jnp.int32)
    values = tags.astype(jnp.float32)
    chosen = jnp.sum(jnp.where(lane == own, values, 0.0), axis=1)
    weighing = (lane == own + experts) | (lane == own + 2 * experts)
    weight = jnp.sum(jnp.where(weighing, values, 0.0), axis=1)
    row = jnp.arange(rows, dtype=jnp.int32)
    earlier = (row[:, None] // MB_ROWS == row[None, :] // MB_ROWS) & (row[None, :] < row[:, None])
    rank = jnp.sum(jnp.where(earlier, chosen[None, :], 0.0), axis=1)
    slot = jnp.arange(blocks * CAP, dtype=jnp.int32)
    same_block = slot[:, None] // CAP == first_block + row[None, :] // MB_ROWS
    same_rank = (slot % CAP).astype(jnp.float32)[:, None] == rank[None, :]
    hits = same_block & same_rank & (chosen[None, :] > 0.5)
    return hits.astype(jnp.bfloat16), weight[:, None]


def matmul(left, right):
    return jnp.dot(left, right, preferred_element_type=jnp.float32)


def expert(rows, gate_proj, up_proj, down_proj):
    gate_sum = matmul(rows, gate_proj)
    up_sum = matmul(rows, up_proj)
    active = (jax.nn.silu(gate_sum) * up_sum).astype(jnp.bfloat16)
    active = lax.optimization_barrier(active)
    return matmul(active, down_proj).astype(jnp.bfloat16)


def body(hidden, norm_gain, router, expert_ids, gate_proj, up_proj, down_proj):
    tokens, features = hidden.shape
    experts = router.shape[1]
    ring = lax.axis_size("ep")
    reach = ring // 2
    own = lax.axis_index("ep") * lax.axis_size("dp") + lax.axis_index("dp")
    normed = normalize(hidden, norm_gain)
    tagged = jnp.concatenate(
        [normed, tag_columns(*dense_weights(normed, router, expert_ids))], axis=1
    )

    sources = [[(0, 0)] if piece == 0 else [] for piece in range(PIECES)]
    blocks = {(0, 0): tagged}
    lower = upper = tagged
    for distance in range(1, reach + 1):
        piece = next(p for p in range(PIECES) if distance <= REACHES[p])
        lower = shift(lower, "ep", 1)
        blocks[distance, 0] = lower
        sources[piece].append((distance, 0))
        if distance < ring - distance:
            upper = shift(upper, "ep", -1)
            blocks[distance, 1] = upper
            sources[piece].append((distance, 1))

    half = features // 2
    gathered = []
    for piece in range(PIECES):
        mine = jnp.concatenate([blocks[source] for source in sources[piece]], axis=0)
        other = shift(mine, "dp", 1)
        count = mine.shape[0] // MB_ROWS
        maps = [
            slot_maps(part[:, features:], own, experts, index * count, 2 * count)
            for index, part in enumerate((mine, other))
        ]
        slots = sum(
            matmul(hits, part[:, :features]) for (hits, _), part in zip(maps, (mine, other))
        ).astype(jnp.bfloat16)
        from_left = shift(slots, "tp", 1)
        from_right = shift(slots, "tp", -1)
        far_head = shift(from_left[:, :half], "tp", 1)
        far_tail = shift(from_right[:, half:], "tp", -1)
        far = jnp.concatenate([far_head, far_tail], axis=1)
        gathered.append((maps, (slots, from_left, from_right, far)))

    sums = {}
    for piece in reversed(range(PIECES)):
        maps, parts = gathered[piece]
        rows = jnp.concatenate(parts, axis=0)
        result = expert(rows, gate_proj[0], up_proj[0], down_proj[0])
        own_part, left_part, right_part, far_part = jnp.split(result, 4, axis=0)
        head = shift(far_part[:, :half], "tp", -1)
        tail = shift(far_part[:, half:], "tp", 1)
        left_head = add(left_part[:, :half], head)
        right_tail = add(right_part[:, half:], tail)
        left_out = jnp.concatenate([left_head, left_part[:, half:]], axis=1)
        right_out = jnp.concatenate([right_part[:, :half], right_tail], axis=1)
        from_right = shift(left_out, "tp", -1)
        from_left = shift(right_out, "tp", 1)
        total = add(own_part, from_right, from_left)
        mine, other = [
            weight
            * lax.dot_general(
                hits, total, (((0,), (0,)), ((), ())), preferred_element_type=jnp.float32
            )
            for hits, weight in maps
        ]
        spread = mine + shift(other.astype(jnp.bfloat16), "dp", 1)
        for index, source in enumerate(sources[piece]):
            sums[source] = spread[index * tokens : (index + 1) * tokens]

    lower = upper = None
    for distance in range(reach, 0, -1):
        terms = [sums[distance, 0]]
        if (distance, 1) in sums:
            terms.append(sums[distance, 1])
        if lower is not None:
            terms[0] = terms[0] + lower
        if upper is not None:
            terms[1] = terms[1] + upper
        terms = lax.optimization_barrier([term.astype(jnp.bfloat16) for term in terms])
        lower = shift(terms[0], "ep", -1)
        if len(terms) > 1:
            upper = shift(terms[1], "ep", 1)
    expert_sum = sums[0, 0] + lower + upper
    return (hidden.astype(jnp.float32) + expert_sum).astype(jnp.bfloat16)


def solution(mesh):
    return jax.shard_map(
        body,
        mesh=mesh,
        in_specs=(
            P(("groups", "ep", "tp", "dp"), None),
            P(),
            P(),
            P(("groups", "ep", "tp", "dp"), None),
            P(("ep", "dp"), None, "tp"),
            P(("ep", "dp"), None, "tp"),
            P(("ep", "dp"), "tp", None),
        ),
        out_specs=P(("groups", "ep", "tp", "dp"), None),
        check_vma=False,
    )
```
